32 devices in a mesh: blk: 2 (over x), wide: 16 (over z, y, core).
Axes of the slice: x: 2, y: 2, z: 4, core: 2. Of those that a mesh axis runs over, the one named last changes fastest.
Arguments:
- volume: float32 [2, 2, 512, 896], P('blk', None, 'wide'), may hold values from -1.6 to 1.6
- path_lengths: float32 [2, 2, 2], replicated, may hold values from 0.5 to 2
- probe: float32 [2, 128, 128], replicated, may hold values from -6 to 6
- measured: bfloat16 [2, 16, 14, 128, 128], P('blk', 'wide'), may hold values from 0.19921875 to 3
- jitter: int32 [2, 2, 16, 14], P(None, 'blk', 'wide'), may hold values from 0 to 15
- step_sizes: float32 [2], replicated, may hold values from 0.02 to 0.2
Outputs:
- new_volume: float32 [2, 2, 512, 896], P('blk', None, 'wide')
- misfit: float32 [], replicated
The draws below stay inside these ranges and needn't reach their ends.
All inputs are finite; a program needn't handle non-finite values.
Results may differ from the reference program's by a relative error of at most 0.0003.
Values sent between devices are 32-bit elements; how exact they have to be, the bound alone decides.
A program may use at most 64 MiB of HBM per device.

```python
import math
import jax
import jax.numpy as jnp
from jax import lax

LAYERS = 2
ROWS_DEV = 32
COLS = 896
PATCH = 128
CSTEP = 64
JIT = 16
PCOLS = 14
HEIGHT = 512
N_BLK = 2
N_WIDE = 16


def with_ends(drawn, stream_key, least, largest):
    extent = drawn.shape
    spot = [jax.random.randint(jax.random.fold_in(stream_key, axis), (), 0, extent[axis]) for axis in range(len(extent))]
    drawn = drawn.at[tuple(spot)].set(least)
    longest = extent.index(max(extent))
    spot[longest] = (spot[longest] + 1) % extent[longest]
    return drawn.at[tuple(spot)].set(largest)


def shard_levels(rng, dims, pieces, smallest, top_value):
    loudness, own = 1.0, jax.random.fold_in(rng, 6)
    for dim, shards_of in pieces:
        draws = jnp.exp(jax.random.uniform(jax.random.fold_in(own, dim), (shards_of,), jnp.float32, smallest / len(pieces), top_value / len(pieces)))
        loudness = loudness * jnp.repeat(draws, dims[dim] // shards_of).reshape([-1 if axis == dim else 1 for axis in range(len(dims))])
    return loudness


def noise(key, dims, scale, bound, shards=(), kind=jnp.bfloat16):
    drawn = jax.random.normal(key, dims, jnp.float32) * scale
    if len(shards) > 0:
        drawn = shard_levels(key, dims, shards, -0.22, 0.18) * drawn
    return jnp.clip(drawn, min=-bound, max=bound).astype(kind)


def setup_inputs(seed: int = 0) -> dict:
    streams_of = jax.random.split(jax.random.key(seed), 7)
    return {
        "volume": noise(streams_of[0], (N_BLK, LAYERS, HEIGHT, COLS), 0.2, 1.6, ((0, 2), (2, 16)), jnp.float32),
        "path_lengths": jnp.clip(jnp.exp(jax.random.uniform(streams_of[1], (N_BLK, N_BLK, LAYERS), jnp.float32, math.log(0.5), math.log(2.0))), 0.5, 2.0),
        "probe": noise(streams_of[2], (2, PATCH, PATCH), 1.0, 6.0, (), jnp.float32),
        "measured": jnp.clip(jnp.exp(math.log(3.0) - 2.7119641 * jax.random.uniform(streams_of[3], (N_BLK, N_WIDE, PCOLS, PATCH, PATCH), jnp.float32) ** shard_levels(streams_of[3], (N_BLK, N_WIDE, PCOLS, PATCH, PATCH), ((0, 2), (1, 16)), -0.2, 0.2)), 0.19921875, 3.0).astype(jnp.bfloat16),
        "jitter": with_ends(jax.random.randint(streams_of[4], (2, N_BLK, N_WIDE, PCOLS), 0, JIT), jax.random.fold_in(streams_of[4], 1), 0, JIT - 1).astype(jnp.int32),
        "step_sizes": jnp.clip(jnp.exp(jax.random.uniform(streams_of[5], (N_BLK,), jnp.float32, math.log(0.02), math.log(0.2))), 0.02, 0.2),
    }


highest = lax.Precision.HIGHEST
floor_value = 0.25

def dft_tables(length):
    grid = jnp.arange(length, dtype=jnp.int32)
    product = grid[:, None] * grid[None, :] % length
    angles = product.astype(jnp.float32) * (2.0 * math.pi / length)
    factor = 1.0 / math.sqrt(length)
    return (jnp.cos(angles) * factor, -jnp.sin(angles) * factor)

def left_apply(table, batch):
    return jnp.einsum('jk,bkl->bjl', table, batch, precision=highest)

def right_apply(batch, table):
    return jnp.einsum('bjk,kl->bjl', batch, table, precision=highest)

def transform(real_in, imag_in, cos_table, sin_table):
    mid_real = left_apply(cos_table, real_in) - left_apply(sin_table, imag_in)
    mid_imag = left_apply(cos_table, imag_in) + left_apply(sin_table, real_in)
    out_real = right_apply(mid_real, cos_table) - right_apply(mid_imag, sin_table)
    out_imag = right_apply(mid_real, sin_table) + right_apply(mid_imag, cos_table)
    return (out_real, out_imag)

def strip_update(strip_real, strip_imaginary, probe, measured, jitter_rows, jitter_cols, row_corner, column_corner):
    patch_len = probe.shape[-1]
    number = measured.shape[0]
    cos_table, sin_table = dft_tables(patch_len)
    starts_row = (row_corner + jitter_rows).astype(jnp.int32)
    starts_col = (column_corner + CSTEP * jnp.arange(number, dtype=jnp.int32) + jitter_cols).astype(jnp.int32)

    def window(image, top, left):
        return lax.dynamic_slice(image, (top, left), (patch_len, patch_len))
    pick = jax.vmap(window, in_axes=(None, 0, 0))
    obj_real = pick(strip_real, starts_row, starts_col)
    obj_imag = pick(strip_imaginary, starts_row, starts_col)
    probe_real = probe[0]
    probe_imag = probe[1]
    wave_real = probe_real * obj_real - probe_imag * obj_imag
    wave_imag = probe_real * obj_imag + probe_imag * obj_real
    far_real, far_imag = transform(wave_real, wave_imag, cos_table, sin_table)
    modulus = jnp.sqrt(far_real * far_real + far_imag * far_imag)
    target = measured.astype(jnp.float32)
    error = modulus - target
    partial_misfit = jnp.sum(error * error)
    ratio = target / jnp.maximum(modulus, floor_value)
    back_real, back_imag = transform(ratio * far_real, ratio * far_imag, cos_table, -sin_table)
    diff_real = back_real - wave_real
    diff_imag = back_imag - wave_imag
    corr_real = probe_real * diff_real + probe_imag * diff_imag
    corr_imag = probe_real * diff_imag - probe_imag * diff_real

    def place(position, sums):
        acc_real, acc_imag = sums
        top = starts_row[position]
        left = starts_col[position]
        acc_real = lax.dynamic_update_slice(acc_real, window(acc_real, top, left) + corr_real[position], (top, left))
        acc_imag = lax.dynamic_update_slice(acc_imag, window(acc_imag, top, left) + corr_imag[position], (top, left))
        return (acc_real, acc_imag)
    zeros = jnp.zeros(strip_real.shape, strip_real.dtype)
    acc_real, acc_imag = lax.fori_loop(0, number, place, (zeros, zeros))
    return (acc_real, acc_imag, partial_misfit)

def reference(volume, path_lengths, probe, measured, jitter, step_sizes):
    projections = jnp.einsum('asl,slhc->ahc', path_lengths, volume, precision=highest)
    margin = PATCH // 2
    row_corner = ROWS_DEV // 4
    column_corner = PATCH // 4 - ROWS_DEV // 4
    height = ROWS_DEV * N_WIDE
    band_rows = 5 * ROWS_DEV
    gradients = []
    total = jnp.zeros((), jnp.float32)
    for angle in range(N_BLK):
        phase = projections[angle]
        obj_real = jnp.pad(jnp.cos(phase), ((2 * ROWS_DEV, 2 * ROWS_DEV), (margin, margin)))
        obj_imag = jnp.pad(jnp.sin(phase), ((2 * ROWS_DEV, 2 * ROWS_DEV), (margin, margin)))
        width_all = obj_real.shape[1]

        def row_step(carry, input_arrays):
            acc_real, acc_imag, running = carry
            strip_index, recorded_row, shaken_rows, shaken_columns = input_arrays
            top = (strip_index * ROWS_DEV).astype(jnp.int32)
            zero_col = jnp.zeros((), jnp.int32)
            strip_real = lax.dynamic_slice(obj_real, (top, zero_col), (band_rows, width_all))
            strip_imaginary = lax.dynamic_slice(obj_imag, (top, zero_col), (band_rows, width_all))
            portion_real, portion_imaginary, part = strip_update(strip_real, strip_imaginary, probe, recorded_row, shaken_rows, shaken_columns, row_corner, column_corner)
            acc_real = lax.dynamic_update_slice(acc_real, lax.dynamic_slice(acc_real, (top, zero_col), (band_rows, width_all)) + portion_real, (top, zero_col))
            acc_imag = lax.dynamic_update_slice(acc_imag, lax.dynamic_slice(acc_imag, (top, zero_col), (band_rows, width_all)) + portion_imaginary, (top, zero_col))
            return ((acc_real, acc_imag, running + part), None)
        input_arrays = (jnp.arange(N_WIDE, dtype=jnp.int32), measured[angle], jitter[0, angle], jitter[1, angle])
        start = (jnp.zeros(obj_real.shape, jnp.float32), jnp.zeros(obj_real.shape, jnp.float32), jnp.zeros((), jnp.float32))
        (acc_real, acc_imag, part), unused = lax.scan(row_step, start, input_arrays)
        total = total + part
        inner_r = slice(2 * ROWS_DEV, 2 * ROWS_DEV + height)
        inner_c = slice(margin, margin + COLS)
        gradients.append(obj_real[inner_r, inner_c] * acc_imag[inner_r, inner_c] - obj_imag[inner_r, inner_c] * acc_real[inner_r, inner_c])
    stacked = jnp.stack(gradients, 0)
    coeffs = step_sizes[:, None, None] * path_lengths
    update = jnp.einsum('asl,ahc->slhc', coeffs, stacked, precision=highest)
    return (volume - update, total)
```

```python
import functools
import math

import jax
import jax.numpy as jnp
import numpy as np
from jax import lax
from jax.experimental import pallas as pl
from jax.experimental.pallas import tpu as pltpu
from jax.sharding import PartitionSpec as P

PATCH = 128
LANES = 128
MESH = pl.DeviceIdType.MESH
F32 = jnp.float32
BF16 = jnp.bfloat16
floor_value = 0.25

PHASE_MOVES = ((2, 8, 32, 0), (1, 0, 32, 24), (-1, 0, 32, 88), (-2, 0, 24, 120))
GRAD_MOVES = ((2, 120, 144, 0), (1, 88, 120, 0), (-1, 24, 56, 0), (-2, 0, 24, 8))
OWN_FIRST = 56
STRIP = 144


def dft_tables(length):
    grid = np.arange(length)
    angles = (grid[:, None] * grid[None, :] % length) * (2.0 * math.pi / length)
    cos = np.cos(angles) / math.sqrt(length)
    sin = -np.sin(angles) / math.sqrt(length)
    left = np.block([[cos, -sin], [sin, cos]])
    tables = []
    for whole in (left, left.T):
        high = whole.astype(jnp.bfloat16)
        low = (whole - high.astype(np.float64)).astype(jnp.bfloat16)
        tables += [high, low]
    return tables


def sin_cos(x):
    turns = jnp.floor(x * (2.0 / math.pi) + (0.5))
    r = x - turns * (1.5703125)
    r = r - turns * (4.837512969970703125e-4)
    r = r - turns * (7.54978995489188216e-8)
    z = r * r
    s = (((-1.9515295891e-4) * z + (8.3321608736e-3)) * z + (-1.6666654611e-1)) * z * r + r
    c = (((2.443315711809948e-5) * z + (-1.388731625493765e-3)) * z + (4.166664568298827e-2)) * z * z
    c = c - (0.5) * z + (1.0)
    quad = turns.astype(jnp.int32)
    odd = (quad & 1) == 1
    sin_out = jnp.where(odd, c, s)
    cos_out = jnp.where(odd, s, c)
    sin_out = jnp.where((quad & 2) == 2, -sin_out, sin_out)
    cos_out = jnp.where(((quad + 1) & 2) == 2, -cos_out, cos_out)
    return sin_out, cos_out


def split(x):
    high = x.astype(BF16)
    return high, (x - high.astype(F32)).astype(BF16)


def dot(a, b):
    return jnp.dot(a, b, preferred_element_type=F32)


def from_left(high, low, x):
    xh, xl = split(x)
    return dot(jnp.concatenate([high, high, low], 1), jnp.concatenate([xh, xl, xh], 0))


def from_right(x, high, low):
    xh, xl = split(x)
    return dot(jnp.concatenate([xh, xl, xh], 1), jnp.concatenate([high, high, low], 0))


def kernel(
    groups, columns, near,
    path_ref, jit_ref, slab_ref, probe_ref, meas_ref, th_ref, tl_ref, rh_ref, rl_ref,
    grad_out, mis_out,
    asend, arecv, ph, objr, obji, gacc, cbuf, gbuf, mis1, mis2,
    a_s, a_r, b_s, b_r, c_s, c_r, d_s, d_r, m1_s, m1_r, m2_s, m2_r,
):
    group = lax.axis_index("blk")
    me = lax.axis_index("wide")
    layers, rows, cols = slab_ref.shape
    tiles = cols // LANES
    far_count = columns // near
    my_near = lax.rem(me, near)
    my_far = me // near
    first_near = me - my_near
    near_all = groups * near
    near_id = group * near + my_near

    def near_device(step):
        other = lax.rem(near_id + step, near_all)
        return (other // near, first_near + lax.rem(other, near))

    def far_device(step):
        return (group, lax.rem(my_far + step, far_count) * near + my_near)

    def there(offset):
        return (me + offset >= 0) & (me + offset < columns)

    barrier = pltpu.get_barrier_semaphore()
    for step in range(1, near_all):
        pl.semaphore_signal(barrier, inc=1, device_id=near_device(step), device_id_type=MESH)
    for step in range(1, far_count):
        pl.semaphore_signal(barrier, inc=1, device_id=far_device(step), device_id_type=MESH)
    for offset, *_ in PHASE_MOVES:
        @pl.when(there(offset))
        def _():
            pl.semaphore_signal(barrier, inc=1, device_id=(group, me + offset), device_id_type=MESH)

    def slab_term(angle, tile):
        total = path_ref[angle, group, 0] * slab_ref[0, :, tile * LANES : (tile + 1) * LANES]
        for layer in range(1, layers):
            total = total + path_ref[angle, group, layer] * slab_ref[layer, :, tile * LANES : (tile + 1) * LANES]
        return total

    for tile in range(tiles):
        for step in range(1, groups):
            asend[step - 1, tile] = slab_term(lax.rem(group + step, groups), tile)
        ph[tile, OWN_FIRST : OWN_FIRST + rows] = slab_term(group, tile)
    zero = jnp.zeros((STRIP, LANES), F32)
    for edge in (0, tiles + 1):
        objr[edge] = zero
        obji[edge] = zero
    gacc[0] = zero
    gacc[1] = zero

    partners = near_all - 1 + far_count - 1
    for offset, *_ in PHASE_MOVES:
        partners = partners + there(offset).astype(jnp.int32)
    pl.semaphore_wait(barrier, partners)

    def remote(src, dst, send, recv, device):
        return pltpu.make_async_remote_copy(
            src_ref=src, dst_ref=dst, send_sem=send, recv_sem=recv, device_id=device, device_id_type=MESH
        )

    def angle_copy(step, tile):
        device = (lax.rem(group + step, groups), me)
        return remote(asend.at[step - 1, tile], arecv.at[step - 1, tile], a_s.at[step - 1, tile], a_r.at[step - 1, tile], device)

    def phase_copy(way, tile):
        offset, lo, hi, at = PHASE_MOVES[way]
        return remote(
            ph.at[tile, pl.ds(OWN_FIRST + lo, hi - lo)], ph.at[tile, pl.ds(at, hi - lo)],
            b_s.at[way, tile], b_r.at[way, tile], (group, me + offset),
        )

    def grad_copy(way, tile):
        offset, lo, hi, at = GRAD_MOVES[way]
        return remote(
            gacc.at[tile + 1, pl.ds(lo, hi - lo)], cbuf.at[way, tile, pl.ds(at, hi - lo)],
            c_s.at[way, tile], c_r.at[way, tile], (group, me + offset),
        )

    def share_copy(step, tile):
        device = (lax.rem(group + step, groups), me)
        return remote(gbuf.at[0, tile], gbuf.at[step, tile], d_s.at[step - 1, tile], d_r.at[step - 1, tile], device)

    def ways(fn, sign):
        for way, (offset, *_) in enumerate(PHASE_MOVES):
            @pl.when(there(sign * offset))
            def _():
                fn(way)

    for tile in range(tiles):
        for step in range(1, groups):
            angle_copy(step, tile).start()

    def spread(tile, carry):
        own = ph[tile, OWN_FIRST : OWN_FIRST + rows]
        for step in range(1, groups):
            angle_copy(step, tile).wait_recv()
            own = own + arecv[step - 1, tile]
        ph[tile, OWN_FIRST : OWN_FIRST + rows] = own
        ways(lambda way: phase_copy(way, tile).start(), 1)
        return carry

    lax.fori_loop(0, tiles, spread, 0)

    row_iota = lax.broadcasted_iota(jnp.int32, (STRIP, LANES), 0)
    grid_row = row_iota + (me * rows - OWN_FIRST)
    inside = (grid_row >= 0) & (grid_row < rows * columns)

    def prepare(tile):
        ways(lambda way: phase_copy(way, tile).wait_recv(), -1)
        s, c = sin_cos(ph[tile])
        objr[tile + 1] = jnp.where(inside, c, 0.0)
        obji[tile + 1] = jnp.where(inside, s, 0.0)

    def finish(tile):
        ways(lambda way: grad_copy(way, tile).wait_recv(), -1)
        total = gacc[tile + 1, OWN_FIRST : OWN_FIRST + rows]
        row = lax.broadcasted_iota(jnp.int32, (rows, LANES), 0)
        for way, (offset, lo, hi, at) in enumerate(GRAD_MOVES):
            ok = (row >= at) & (row < at + hi - lo) & there(-offset)
            total = total + jnp.where(ok, cbuf[way, tile], 0.0)
        gbuf[0, tile] = total
        for step in range(1, groups):
            share_copy(step, tile).start()

    lane = lax.broadcasted_iota(jnp.int32, (STRIP, LANES), 1)
    row16 = lax.broadcasted_iota(jnp.int32, (STRIP - PATCH, LANES), 0)
    extra = STRIP - PATCH

    def pair(p, misfit):
        @pl.when(p + 1 < tiles)
        def _():
            prepare(p + 1)

        waves, objects, probes, shifts = [], [], [], []
        for half in range(2):
            position = 2 * p + half
            jr = jit_ref[0, position]
            start = jit_ref[1, position] + (PATCH - 40 if half == 0 else PATCH // 2 - 40)
            keep = lane >= start

            def wrapped(image):
                tall = jnp.where(keep, image[p + half], image[p + half + 1])
                top = jnp.where(row16 >= jr, tall[:extra], tall[PATCH:])
                return jnp.concatenate([top, tall[extra:PATCH]], 0)

            o_r, o_i = wrapped(objr), wrapped(obji)
            p_r = pltpu.roll(pltpu.roll(probe_ref[0], jr, 0), start, 1)
            p_i = pltpu.roll(pltpu.roll(probe_ref[1], jr, 0), start, 1)
            waves.append(jnp.concatenate([p_r * o_r - p_i * o_i, p_r * o_i + p_i * o_r], 0))
            objects.append((o_r, o_i))
            probes.append((p_r, p_i))
            shifts.append((jr, keep))
        th, tl, rh, rl = th_ref[...], tl_ref[...], rh_ref[...], rl_ref[...]
        wave = jnp.concatenate(waves, 1)

        def restack(x):
            upper = jnp.concatenate([x[:PATCH, :PATCH], x[PATCH:, :PATCH]], 1)
            lower = jnp.concatenate([x[:PATCH, PATCH:], x[PATCH:, PATCH:]], 1)
            return jnp.concatenate([upper, lower], 0)

        far = from_right(restack(from_left(th, tl, wave)), rh, rl)
        f_r, f_i = far[:, :PATCH], far[:, PATCH:]
        square = f_r * f_r + f_i * f_i
        inverse = lax.rsqrt(jnp.maximum(square, (1e-35)))
        target = meas_ref[pl.ds(2 * p, 2)].reshape(2 * PATCH, PATCH).astype(F32)
        error = square * inverse - target
        misfit = misfit + jnp.sum((error * error).reshape(2 * PATCH // 8, 8, PATCH), axis=0)
        ratio = target * jnp.minimum(inverse, (1.0 / floor_value))
        level = jnp.concatenate([ratio * f_r, ratio * f_i], 1)
        back = from_left(rh, rl, restack(from_right(level, th, tl)))
        diff = back - wave
        parts = []
        for half in range(2):
            d = diff[:, half * PATCH : (half + 1) * PATCH]
            d_r, d_i = d[:PATCH], d[PATCH:]
            (p_r, p_i), (o_r, o_i), (jr, keep) = probes[half], objects[half], shifts[half]
            c_re = p_r * d_r + p_i * d_i
            c_im = p_r * d_i - p_i * d_r
            g = o_r * c_im - o_i * c_re
            below = row16 >= jr
            tall = jnp.concatenate(
                [jnp.where(below, g[:extra], 0.0), g[extra:], jnp.where(below, 0.0, g[:extra])], 0
            )
            parts.append((jnp.where(keep, tall, 0.0), jnp.where(keep, 0.0, tall)))
        gacc[p] = gacc[p] + parts[0][0]
        gacc[p + 1] = gacc[p + 1] + (parts[0][1] + parts[1][0])
        gacc[p + 2] = parts[1][1]

        @pl.when(p >= 1)
        def _():
            ways(lambda way: grad_copy(way, p - 1).start(), 1)

        @pl.when(p >= 3)
        def _():
            finish(p - 3)

        return misfit

    prepare(0)
    misfit = lax.fori_loop(0, tiles, pair, jnp.zeros((8, PATCH), F32))
    ways(lambda way: grad_copy(way, tiles - 1).start(), 1)

    mis1[near_id] = misfit

    def near_copy(step):
        return remote(mis1.at[near_id], mis1.at[near_id], m1_s.at[step - 1], m1_r.at[step - 1], near_device(step))

    def far_copy(step):
        return remote(mis2.at[my_far], mis2.at[my_far], m2_s.at[step - 1], m2_r.at[step - 1], far_device(step))

    for step in range(1, near_all):
        near_copy(step).start()
    finish(tiles - 3)
    for step in range(1, near_all):
        near_copy(step).wait_recv()
    mis2[my_far] = jnp.sum(mis1[...], axis=0)
    for step in range(1, far_count):
        far_copy(step).start()
    finish(tiles - 2)
    finish(tiles - 1)

    def collect(tile, carry):
        for step in range(1, groups):
            share_copy(step, tile).wait_recv()
            angle_copy(step, tile).wait_send()
            share_copy(step, tile).wait_send()
        ways(lambda way: phase_copy(way, tile).wait_send(), 1)
        ways(lambda way: grad_copy(way, tile).wait_send(), 1)
        return carry

    lax.fori_loop(0, tiles, collect, 0)
    for tile in range(tiles):
        for step in range(groups):
            angle = lax.rem(group - step + groups, groups)
            grad_out[angle, :, tile * LANES : (tile + 1) * LANES] = gbuf[step, tile]
    for step in range(1, near_all):
        near_copy(step).wait_send()
    for step in range(1, far_count):
        far_copy(step).wait_recv()
    total = jnp.sum(mis2[...], axis=0)
    mis_out[...] = jnp.sum(total, keepdims=True)
    for step in range(1, far_count):
        far_copy(step).wait_send()


def body(mesh, volume, path_lengths, probe, measured, jitter, step_sizes):
    groups, columns = mesh.shape["blk"], mesh.shape["wide"]
    near = math.gcd(columns, 4)
    slab = volume[0]
    layers, rows, cols = slab.shape
    tiles = cols // LANES
    tables = [jnp.asarray(t) for t in dft_tables(probe.shape[-1])]
    vmem = pl.BlockSpec(memory_space=pltpu.VMEM)
    smem = pl.BlockSpec(memory_space=pltpu.SMEM)
    sem = pltpu.SemaphoreType.DMA
    others = max(groups - 1, 1)
    grads, misfit = pl.pallas_call(
        functools.partial(kernel, groups, columns, near),
        out_shape=(
            jax.ShapeDtypeStruct((groups, rows, cols), F32),
            jax.ShapeDtypeStruct((1, 1), F32),
        ),
        in_specs=[smem, smem] + [vmem] * 7,
        out_specs=(vmem, vmem),
        scratch_shapes=[
            pltpu.VMEM((others, tiles, rows, LANES), F32),
            pltpu.VMEM((others, tiles, rows, LANES), F32),
            pltpu.VMEM((tiles, STRIP, LANES), F32),
            pltpu.VMEM((tiles + 2, STRIP, LANES), F32),
            pltpu.VMEM((tiles + 2, STRIP, LANES), F32),
            pltpu.VMEM((tiles + 2, STRIP, LANES), F32),
            pltpu.VMEM((4, tiles, rows, LANES), F32),
            pltpu.VMEM((groups, tiles, rows, LANES), F32),
            pltpu.VMEM((groups * near, 8, LANES), F32),
            pltpu.VMEM((columns // near, 8, LANES), F32),
            sem((others, tiles)), sem((others, tiles)),
            sem((4, tiles)), sem((4, tiles)),
            sem((4, tiles)), sem((4, tiles)),
            sem((others, tiles)), sem((others, tiles)),
            sem((groups * near,)), sem((groups * near,)),
            sem((columns // near,)), sem((columns // near,)),
        ],
        compiler_params=pltpu.CompilerParams(collective_id=0, has_side_effects=True),
    )(path_lengths, jitter[:, 0, 0], slab, probe, measured[0, 0], *tables)
    group = lax.axis_index("blk")
    own_paths = lax.dynamic_index_in_dim(path_lengths, group, 1, keepdims=False)
    coeffs = step_sizes[:, None] * own_paths
    update = coeffs[0][:, None, None] * grads[0]
    for angle in range(1, groups):
        update = update + coeffs[angle][:, None, None] * grads[angle]
    return ((slab - update)[None], misfit[0, 0])


def solution(mesh):
    in_specs = (
        P("blk", None, "wide", None),
        P(),
        P(),
        P("blk", "wide", None, None, None),
        P(None, "blk", "wide", None),
        P(),
    )
    out_specs = (P("blk", None, "wide", None), P())
    return jax.shard_map(
        functools.partial(body, mesh), mesh=mesh, in_specs=in_specs, out_specs=out_specs, check_vma=False
    )
```

```python
import functools
import math

import jax
import jax.numpy as jnp
import numpy as np
from jax import lax
from jax.experimental import pallas as pl
from jax.experimental.pallas import tpu as pltpu
from jax.sharding import PartitionSpec as P

PATCH = 128
LANES = 128
MESH = pl.DeviceIdType.MESH
F32 = jnp.float32
BF16 = jnp.bfloat16
floor_value = 0.25

PHASE_MOVES = ((2, 8, 32, 0), (1, 0, 32, 24), (-1, 0, 32, 88), (-2, 0, 24, 120))
GRAD_MOVES = ((2, 120, 144, 0), (1, 88, 120, 0), (-1, 24, 56, 0), (-2, 0, 24, 8))
OWN_FIRST = 56
STRIP = 144


def dft_tables(length):
    grid = np.arange(length)
    angles = (grid[:, None] * grid[None, :] % length) * (2.0 * math.pi / length)
    cos = np.cos(angles) / math.sqrt(length)
    sin = -np.sin(angles) / math.sqrt(length)
    left = np.block([[cos, -sin], [sin, cos]])
    tables = []
    for whole in (left, left.T):
        high = whole.astype(jnp.bfloat16)
        low = (whole - high.astype(np.float64)).astype(jnp.bfloat16)
        tables += [high, low]
    return tables


def sin_cos(x):
    turns = jnp.floor(x * (2.0 / math.pi) + (0.5))
    r = x - turns * (1.5703125)
    r = r - turns * (4.837512969970703125e-4)
    r = r - turns * (7.54978995489188216e-8)
    z = r * r
    s = (((-1.9515295891e-4) * z + (8.3321608736e-3)) * z + (-1.6666654611e-1)) * z * r + r
    c = (((2.443315711809948e-5) * z + (-1.388731625493765e-3)) * z + (4.166664568298827e-2)) * z * z
    c = c - (0.5) * z + (1.0)
    quad = turns.astype(jnp.int32)
    odd = (quad & 1) == 1
    sin_out = jnp.where(odd, c, s)
    cos_out = jnp.where(odd, s, c)
    sin_out = jnp.where((quad & 2) == 2, -sin_out, sin_out)
    cos_out = jnp.where(((quad + 1) & 2) == 2, -cos_out, cos_out)
    return sin_out, cos_out


def split(x):
    high = x.astype(BF16)
    return high, (x - high.astype(F32)).astype(BF16)


def dot(a, b):
    return jnp.dot(a, b, preferred_element_type=F32)


def from_left(high, low, x):
    xh, xl = split(x)
    return dot(jnp.concatenate([high, high, low], 1), jnp.concatenate([xh, xl, xh], 0))


def from_right(x, high, low):
    xh, xl = split(x)
    return dot(jnp.concatenate([xh, xl, xh], 1), jnp.concatenate([high, high, low], 0))


def kernel(
    groups, columns, near,
    path_ref, jit_ref, step_ref, slab_hbm, probe_hbm, meas_hbm, th_hbm, tl_hbm, rh_hbm, rl_hbm,
    new_out, mis_out,
    slab_ref, probe_ref, meas_ref, th_ref, tl_ref, rh_ref, rl_ref, in_sem,
    wave_ref, level_ref, own_ref, asend, arecv, ph, objr, obji, gacc, cbuf, gbuf, mis1, mis2,
    a_s, a_r, b_s, b_r, c_s, c_r, d_s, d_r, m1_s, m1_r, m2_s, m2_r,
):
    group = lax.axis_index("blk")
    me = lax.axis_index("wide")
    layers, rows, cols = slab_ref.shape
    tiles = cols // LANES
    far_count = columns // near
    my_near = lax.rem(me, near)
    my_far = me // near
    first_near = me - my_near
    near_all = groups * near
    near_id = group * near + my_near

    def near_device(step):
        other = lax.rem(near_id + step, near_all)
        return (other // near, first_near + lax.rem(other, near))

    def far_device(step):
        return (group, lax.rem(my_far + step, far_count) * near + my_near)

    def there(offset):
        return (me + offset >= 0) & (me + offset < columns)

    loads = [
        pltpu.make_async_copy(src, dst, in_sem.at[i])
        for i, (src, dst) in enumerate((
            (slab_hbm, slab_ref), (probe_hbm, probe_ref), (meas_hbm, meas_ref),
            (th_hbm, th_ref), (tl_hbm, tl_ref), (rh_hbm, rh_ref), (rl_hbm, rl_ref),
        ))
    ]
    loads[0].start()
    barrier = pltpu.get_barrier_semaphore()
    for step in range(1, near_all):
        pl.semaphore_signal(barrier, inc=1, device_id=near_device(step), device_id_type=MESH)
    for step in range(1, far_count):
        pl.semaphore_signal(barrier, inc=1, device_id=far_device(step), device_id_type=MESH)
    for offset, *_ in PHASE_MOVES:
        @pl.when(there(offset))
        def _():
            pl.semaphore_signal(barrier, inc=1, device_id=(group, me + offset), device_id_type=MESH)

    def slab_term(angle, tile):
        total = path_ref[angle, group, 0] * slab_ref[0, :, tile * LANES : (tile + 1) * LANES]
        for layer in range(1, layers):
            total = total + path_ref[angle, group, layer] * slab_ref[layer, :, tile * LANES : (tile + 1) * LANES]
        return total

    for load in loads[1:]:
        load.start()
    loads[0].wait()
    for tile in range(tiles):
        for step in range(1, groups):
            asend[step - 1, tile] = slab_term(lax.rem(group + step, groups), tile)
        ph[tile, OWN_FIRST : OWN_FIRST + rows] = slab_term(group, tile)
    zero = jnp.zeros((STRIP, LANES), F32)
    for edge in (0, tiles + 1):
        objr[edge] = zero
        obji[edge] = zero
    gacc[0] = zero
    gacc[1] = zero

    partners = near_all - 1 + far_count - 1
    for offset, *_ in PHASE_MOVES:
        partners = partners + there(offset).astype(jnp.int32)
    pl.semaphore_wait(barrier, partners)

    def remote(src, dst, send, recv, device):
        return pltpu.make_async_remote_copy(
            src_ref=src, dst_ref=dst, send_sem=send, recv_sem=recv, device_id=device, device_id_type=MESH
        )

    def angle_copy(step, tile):
        device = (lax.rem(group + step, groups), me)
        return remote(asend.at[step - 1, tile], arecv.at[step - 1, tile], a_s.at[step - 1, tile], a_r.at[step - 1, tile], device)

    def phase_copy(way, tile):
        offset, lo, hi, at = PHASE_MOVES[way]
        return remote(
            ph.at[tile, pl.ds(OWN_FIRST + lo, hi - lo)], ph.at[tile, pl.ds(at, hi - lo)],
            b_s.at[way, tile], b_r.at[way, tile], (group, me + offset),
        )

    def grad_copy(way, tile):
        offset, lo, hi, at = GRAD_MOVES[way]
        return remote(
            gacc.at[tile + 1, pl.ds(lo, hi - lo)], cbuf.at[way, tile, pl.ds(at, hi - lo)],
            c_s.at[way, tile], c_r.at[way, tile], (group, me + offset),
        )

    def share_copy(step, tile):
        device = (lax.rem(group + step, groups), me)
        return remote(gbuf.at[0, tile], gbuf.at[step, tile], d_s.at[step - 1, tile], d_r.at[step - 1, tile], device)

    def ways(fn, sign):
        for way, (offset, *_) in enumerate(PHASE_MOVES):
            @pl.when(there(sign * offset))
            def _():
                fn(way)

    for tile in range(tiles):
        for step in range(1, groups):
            angle_copy(step, tile).start()

    def spread(tile, carry):
        own = ph[tile, OWN_FIRST : OWN_FIRST + rows]
        for step in range(1, groups):
            angle_copy(step, tile).wait_recv()
            own = own + arecv[step - 1, tile]
        ph[tile, OWN_FIRST : OWN_FIRST + rows] = own
        ways(lambda way: phase_copy(way, tile).start(), 1)
        return carry

    lax.fori_loop(0, tiles, spread, 0)

    row_iota = lax.broadcasted_iota(jnp.int32, (STRIP, LANES), 0)
    grid_row = row_iota + (me * rows - OWN_FIRST)
    inside = (grid_row >= 0) & (grid_row < rows * columns)

    def prepare(tile):
        ways(lambda way: phase_copy(way, tile).wait_recv(), -1)
        s, c = sin_cos(ph[tile])
        objr[tile + 1] = jnp.where(inside, c, 0.0)
        obji[tile + 1] = jnp.where(inside, s, 0.0)

    def finish(tile):
        ways(lambda way: grad_copy(way, tile).wait_recv(), -1)
        total = gacc[tile + 1, OWN_FIRST : OWN_FIRST + rows]
        row = lax.broadcasted_iota(jnp.int32, (rows, LANES), 0)
        for way, (offset, lo, hi, at) in enumerate(GRAD_MOVES):
            ok = (row >= at) & (row < at + hi - lo) & there(-offset)
            total = total + jnp.where(ok, cbuf[way, tile], 0.0)
        gbuf[0, tile] = total
        for step in range(1, groups):
            share_copy(step, tile).start()

    lane = lax.broadcasted_iota(jnp.int32, (STRIP, LANES), 1)
    row16 = lax.broadcasted_iota(jnp.int32, (STRIP - PATCH, LANES), 0)
    extra = STRIP - PATCH

    def restack(x):
        upper = jnp.concatenate([x[:PATCH, :PATCH], x[PATCH:, :PATCH]], 1)
        lower = jnp.concatenate([x[:PATCH, PATCH:], x[PATCH:, PATCH:]], 1)
        return jnp.concatenate([upper, lower], 0)

    def shift_of(p, half):
        position = 2 * p + half
        return jit_ref[0, position], jit_ref[1, position] + (PATCH - 40 if half == 0 else PATCH // 2 - 40)

    def forward(p):
        slot = p % 2
        waves = []
        for half in range(2):
            jr, start = shift_of(p, half)
            keep = lane >= start

            def wrapped(image):
                tall = jnp.where(keep, image[p + half], image[p + half + 1])
                top = jnp.where(row16 >= jr, tall[:extra], tall[PATCH:])
                return jnp.concatenate([top, tall[extra:PATCH]], 0)

            o_r, o_i = wrapped(objr), wrapped(obji)
            p_r = pltpu.roll(pltpu.roll(probe_ref[0], jr, 0), start, 1)
            p_i = pltpu.roll(pltpu.roll(probe_ref[1], jr, 0), start, 1)
            waves.append(jnp.concatenate([p_r * o_r - p_i * o_i, p_r * o_i + p_i * o_r], 0))
            for index, value in enumerate((o_r, o_i, p_r, p_i)):
                own_ref[slot, half, index] = value
        wave = jnp.concatenate(waves, 1)
        wave_ref[slot] = wave
        far = from_right(restack(from_left(th_ref[...], tl_ref[...], wave)), rh_ref[...], rl_ref[...])
        f_r, f_i = far[:, :PATCH], far[:, PATCH:]
        square = f_r * f_r + f_i * f_i
        inverse = lax.rsqrt(jnp.maximum(square, (1e-35)))
        target = meas_ref[2 * p : 2 * p + 2].reshape(2 * PATCH, PATCH).astype(F32)
        error = square * inverse - target
        ratio = target * jnp.minimum(inverse, (1.0 / floor_value))
        level_ref[slot] = jnp.concatenate([ratio * f_r, ratio * f_i], 1)
        return jnp.sum((error * error).reshape(2 * PATCH // 8, 8, PATCH), axis=0)

    def backward(p):
        slot = p % 2
        back = from_left(rh_ref[...], rl_ref[...], restack(from_right(level_ref[slot], th_ref[...], tl_ref[...])))
        diff = back - wave_ref[slot]
        parts = []
        for half in range(2):
            jr, start = shift_of(p, half)
            keep = lane >= start
            d = diff[:, half * PATCH : (half + 1) * PATCH]
            d_r, d_i = d[:PATCH], d[PATCH:]
            o_r, o_i, p_r, p_i = (own_ref[slot, half, index] for index in range(4))
            c_re = p_r * d_r + p_i * d_i
            c_im = p_r * d_i - p_i * d_r
            g = o_r * c_im - o_i * c_re
            below = row16 >= jr
            tall = jnp.concatenate(
                [jnp.where(below, g[:extra], 0.0), g[extra:], jnp.where(below, 0.0, g[:extra])], 0
            )
            parts.append((jnp.where(keep, tall, 0.0), jnp.where(keep, 0.0, tall)))
        gacc[p] = gacc[p] + parts[0][0]
        gacc[p + 1] = gacc[p + 1] + (parts[0][1] + parts[1][0])
        gacc[p + 2] = parts[1][1]

    def near_copy(step):
        return remote(mis1.at[near_id], mis1.at[near_id], m1_s.at[step - 1], m1_r.at[step - 1], near_device(step))

    def far_copy(step):
        return remote(mis2.at[my_far], mis2.at[my_far], m2_s.at[step - 1], m2_r.at[step - 1], far_device(step))

    prepare(0)
    prepare(1)
    for load in loads[1:]:
        load.wait()
    misfit = forward(0)
    for p in range(tiles):
        if p + 2 < tiles:
            prepare(p + 2)
        backward(p)
        if p + 1 < tiles:
            misfit = misfit + forward(p + 1)
        if p >= 1:
            ways(lambda way: grad_copy(way, p - 1).start(), 1)
        if p == tiles - 2:
            mis1[near_id] = jnp.sum(misfit, axis=0, keepdims=True)
            for step in range(1, near_all):
                near_copy(step).start()
        if p >= 3:
            finish(p - 3)
    ways(lambda way: grad_copy(way, tiles - 1).start(), 1)
    for step in range(1, near_all):
        near_copy(step).wait_recv()
    mis2[my_far] = jnp.sum(mis1[...], axis=0)
    for step in range(1, far_count):
        far_copy(step).start()
    finish(tiles - 3)
    finish(tiles - 2)
    finish(tiles - 1)

    def collect(tile, carry):
        for step in range(1, groups):
            angle_copy(step, tile).wait_send()
            share_copy(step, tile).wait_send()
        ways(lambda way: phase_copy(way, tile).wait_send(), 1)
        ways(lambda way: grad_copy(way, tile).wait_send(), 1)
        return carry

    for tile in range(tiles):
        span = slice(tile * LANES, (tile + 1) * LANES)
        news = [jnp.zeros((rows, LANES), F32)] * layers
        for step in range(groups):
            if step > 0:
                share_copy(step, tile).wait_recv()
            angle = lax.rem(group - step + groups, groups)
            for layer in range(layers):
                news[layer] = news[layer] + (step_ref[angle] * path_ref[angle, group, layer]) * gbuf[step, tile]
        for layer in range(layers):
            new_out[0, layer, :, span] = news[layer]
    for step in range(1, near_all):
        near_copy(step).wait_send()
    for step in range(1, far_count):
        far_copy(step).wait_recv()
    total = jnp.sum(mis2[...], axis=0)
    mis_out[...] = jnp.sum(total, keepdims=True)
    for step in range(1, far_count):
        far_copy(step).wait_send()
    lax.fori_loop(0, tiles, collect, 0)


def body(mesh, volume, path_lengths, probe, measured, jitter, step_sizes):
    groups, columns = mesh.shape["blk"], mesh.shape["wide"]
    near = math.gcd(columns, 4)
    slab = volume[0]
    layers, rows, cols = slab.shape
    tiles = cols // LANES
    tables = [jnp.asarray(t) for t in dft_tables(probe.shape[-1])]
    vmem = pl.BlockSpec(memory_space=pltpu.VMEM)
    smem = pl.BlockSpec(memory_space=pltpu.SMEM)
    hbm = pl.BlockSpec(memory_space=pl.ANY)
    sem = pltpu.SemaphoreType.DMA
    loaded = [slab, probe, measured[0, 0], *tables]
    others = max(groups - 1, 1)
    new, misfit = pl.pallas_call(
        functools.partial(kernel, groups, columns, near),
        out_shape=(
            jax.ShapeDtypeStruct((1, layers, rows, cols), F32),
            jax.ShapeDtypeStruct((1, 1), F32),
        ),
        in_specs=[smem] * 3 + [hbm] * 7,
        out_specs=(vmem, vmem),
        scratch_shapes=[
            *(pltpu.VMEM(x.shape, x.dtype) for x in loaded),
            sem((len(loaded),)),
            pltpu.VMEM((2, 2 * PATCH, 2 * PATCH), F32),
            pltpu.VMEM((2, 2 * PATCH, 2 * PATCH), F32),
            pltpu.VMEM((2, 2, 4, PATCH, PATCH), F32),
            pltpu.VMEM((others, tiles, rows, LANES), F32),
            pltpu.VMEM((others, tiles, rows, LANES), F32),
            pltpu.VMEM((tiles, STRIP, LANES), F32),
            pltpu.VMEM((tiles + 2, STRIP, LANES), F32),
            pltpu.VMEM((tiles + 2, STRIP, LANES), F32),
            pltpu.VMEM((tiles + 2, STRIP, LANES), F32),
            pltpu.VMEM((4, tiles, rows, LANES), F32),
            pltpu.VMEM((groups, tiles, rows, LANES), F32),
            pltpu.VMEM((groups * near, 1, LANES), F32),
            pltpu.VMEM((columns // near, 1, LANES), F32),
            sem((others, tiles)), sem((others, tiles)),
            sem((4, tiles)), sem((4, tiles)),
            sem((4, tiles)), sem((4, tiles)),
            sem((others, tiles)), sem((others, tiles)),
            sem((groups * near,)), sem((groups * near,)),
            sem((columns // near,)), sem((columns // near,)),
        ],
        compiler_params=pltpu.CompilerParams(collective_id=0, has_side_effects=True),
    )(path_lengths, jitter[:, 0, 0], step_sizes, *loaded)
    return (volume - new, misfit[0, 0])


def solution(mesh):
    in_specs = (
        P("blk", None, "wide", None),
        P(),
        P(),
        P("blk", "wide", None, None, None),
        P(None, "blk", "wide", None),
        P(),
    )
    out_specs = (P("blk", None, "wide", None), P())
    return jax.shard_map(
        functools.partial(body, mesh), mesh=mesh, in_specs=in_specs, out_specs=out_specs, check_vma=False
    )
```

```python
import functools
import math

import jax
import jax.numpy as jnp
import numpy as np
from jax import lax
from jax.experimental import pallas as pl
from jax.experimental.pallas import tpu as pltpu
from jax.sharding import PartitionSpec as P

PATCH = 128
LANES = 128
MESH = pl.DeviceIdType.MESH
F32 = jnp.float32
BF16 = jnp.bfloat16
floor_value = 0.25

PHASE_MOVES = ((2, 8, 32, 0), (1, 0, 32, 24), (-1, 0, 32, 88), (-2, 0, 24, 120))
GRAD_MOVES = ((2, 120, 144, 0), (1, 88, 120, 0), (-1, 24, 56, 0), (-2, 0, 24, 8))
OWN_FIRST = 56
STRIP = 144


def dft_tables(length):
    grid = np.arange(length)
    angles = (grid[:, None] * grid[None, :] % length) * (2.0 * math.pi / length)
    cos = np.cos(angles) / math.sqrt(length)
    sin = -np.sin(angles) / math.sqrt(length)
    left = np.block([[cos, -sin], [sin, cos]])
    tables = []
    for whole in (left, left.T):
        high = whole.astype(jnp.bfloat16)
        low = (whole - high.astype(np.float64)).astype(jnp.bfloat16)
        tables += [high, low]
    return tables


def sin_cos(x):
    turns = jnp.floor(x * (2.0 / math.pi) + (0.5))
    r = x - turns * (1.5703125)
    r = r - turns * (4.837512969970703125e-4)
    r = r - turns * (7.54978995489188216e-8)
    z = r * r
    s = (((-1.9515295891e-4) * z + (8.3321608736e-3)) * z + (-1.6666654611e-1)) * z * r + r
    c = (((2.443315711809948e-5) * z + (-1.388731625493765e-3)) * z + (4.166664568298827e-2)) * z * z
    c = c - (0.5) * z + (1.0)
    quad = turns.astype(jnp.int32)
    odd = (quad & 1) == 1
    sin_out = jnp.where(odd, c, s)
    cos_out = jnp.where(odd, s, c)
    sin_out = jnp.where((quad & 2) == 2, -sin_out, sin_out)
    cos_out = jnp.where(((quad + 1) & 2) == 2, -cos_out, cos_out)
    return sin_out, cos_out


def split(x):
    high = x.astype(BF16)
    return high, (x - high.astype(F32)).astype(BF16)


def dot(a, b):
    return jnp.dot(a, b, preferred_element_type=F32)


def from_left(high, low, x):
    xh, xl = split(x)
    return dot(jnp.concatenate([high, high, low], 1), jnp.concatenate([xh, xl, xh], 0))


def from_right(x, high, low):
    xh, xl = split(x)
    return dot(jnp.concatenate([xh, xl, xh], 1), jnp.concatenate([high, high, low], 0))


def kernel(
    groups, columns, near,
    path_ref, jit_ref, step_ref, slab_hbm, probe_hbm, meas_hbm, th_hbm, tl_hbm, rh_hbm, rl_hbm,
    new_out, mis_out,
    slab_ref, probe_ref, meas_ref, th_ref, tl_ref, rh_ref, rl_ref, in_sem,
    wave_ref, level_ref, own_ref, asend, arecv, ph, objr, obji, gacc, cbuf, gbuf, mis1, mis2,
    a_s, a_r, b_s, b_r, c_s, c_r, d_s, d_r, m1_s, m1_r, m2_s, m2_r,
):
    group = lax.axis_index("blk")
    me = lax.axis_index("wide")
    layers, rows, cols = slab_ref.shape
    tiles = cols // LANES
    far_count = columns // near
    my_near = lax.rem(me, near)
    my_far = me // near
    first_near = me - my_near
    near_all = groups * near
    near_id = group * near + my_near

    def near_device(step):
        other = lax.rem(near_id + step, near_all)
        return (other // near, first_near + lax.rem(other, near))

    def far_device(step):
        return (group, lax.rem(my_far + step, far_count) * near + my_near)

    def there(offset):
        return (me + offset >= 0) & (me + offset < columns)

    loads = [
        pltpu.make_async_copy(src, dst, in_sem.at[i])
        for i, (src, dst) in enumerate((
            (slab_hbm, slab_ref), (probe_hbm, probe_ref), (meas_hbm, meas_ref),
            (th_hbm, th_ref), (tl_hbm, tl_ref), (rh_hbm, rh_ref), (rl_hbm, rl_ref),
        ))
    ]
    loads[0].start()
    barrier = pltpu.get_barrier_semaphore()
    for step in range(1, near_all):
        pl.semaphore_signal(barrier, inc=1, device_id=near_device(step), device_id_type=MESH)
    for step in range(1, far_count):
        pl.semaphore_signal(barrier, inc=1, device_id=far_device(step), device_id_type=MESH)
    for offset, *_ in PHASE_MOVES:
        @pl.when(there(offset))
        def _():
            pl.semaphore_signal(barrier, inc=1, device_id=(group, me + offset), device_id_type=MESH)

    def slab_term(angle, tile):
        total = path_ref[angle, group, 0] * slab_ref[0, :, tile * LANES : (tile + 1) * LANES]
        for layer in range(1, layers):
            total = total + path_ref[angle, group, layer] * slab_ref[layer, :, tile * LANES : (tile + 1) * LANES]
        return total

    for load in loads[1:]:
        load.start()
    loads[0].wait()
    for tile in range(tiles):
        for step in range(1, groups):
            asend[step - 1, tile] = slab_term(lax.rem(group + step, groups), tile)
        ph[tile, OWN_FIRST : OWN_FIRST + rows] = slab_term(group, tile)
    zero = jnp.zeros((STRIP, LANES), F32)
    for edge in (0, tiles + 1):
        objr[edge] = zero
        obji[edge] = zero
    gacc[0] = zero
    gacc[1] = zero

    partners = near_all - 1 + far_count - 1
    for offset, *_ in PHASE_MOVES:
        partners = partners + there(offset).astype(jnp.int32)
    pl.semaphore_wait(barrier, partners)

    def remote(src, dst, send, recv, device):
        return pltpu.make_async_remote_copy(
            src_ref=src, dst_ref=dst, send_sem=send, recv_sem=recv, device_id=device, device_id_type=MESH
        )

    def angle_copy(step, tile):
        device = (lax.rem(group + step, groups), me)
        return remote(asend.at[step - 1, tile], arecv.at[step - 1, tile], a_s.at[step - 1, tile], a_r.at[step - 1, tile], device)

    def phase_copy(way, tile):
        offset, lo, hi, at = PHASE_MOVES[way]
        return remote(
            ph.at[tile, pl.ds(OWN_FIRST + lo, hi - lo)], ph.at[tile, pl.ds(at, hi - lo)],
            b_s.at[way, tile], b_r.at[way, tile], (group, me + offset),
        )

    def grad_copy(way, tile):
        offset, lo, hi, at = GRAD_MOVES[way]
        return remote(
            gacc.at[tile + 1, pl.ds(lo, hi - lo)], cbuf.at[way, tile, pl.ds(at, hi - lo)],
            c_s.at[way, tile], c_r.at[way, tile], (group, me + offset),
        )

    def share_copy(step, tile):
        device = (lax.rem(group + step, groups), me)
        return remote(gbuf.at[0, tile], gbuf.at[step, tile], d_s.at[step - 1, tile], d_r.at[step - 1, tile], device)

    def ways(fn, sign):
        for way, (offset, *_) in enumerate(PHASE_MOVES):
            @pl.when(there(sign * offset))
            def _():
                fn(way)

    odd = lax.rem(me, 2) == 1

    def sent(fn):
        for way, on in ((1, me + 1 < columns), (2, me >= 1), (0, ~odd & (me + 2 < columns)), (3, odd & (me >= 2))):
            @pl.when(on)
            def _():
                fn(way)

    def relayed(fn, tile):
        for on, first, src, dst, send, way, device in (
            (~odd & (me >= 2), 1, 32, 0, 3, 0, me + 1),
            (odd & (me + 1 < columns), 2, 88, 120, 0, 3, me - 1),
        ):
            @pl.when(on)
            def _():
                fn(first, remote(
                    ph.at[tile, pl.ds(src, 24)], ph.at[tile, pl.ds(dst, 24)],
                    b_s.at[send, tile], b_r.at[way, tile], (group, device),
                ))

    def relay(tile):
        def go(first, copy):
            phase_copy(first, tile).wait_recv()
            copy.start()

        relayed(go, tile)

    for tile in range(tiles):
        for step in range(1, groups):
            angle_copy(step, tile).start()

    def spread(tile, carry):
        own = ph[tile, OWN_FIRST : OWN_FIRST + rows]
        for step in range(1, groups):
            angle_copy(step, tile).wait_recv()
            own = own + arecv[step - 1, tile]
        ph[tile, OWN_FIRST : OWN_FIRST + rows] = own
        sent(lambda way: phase_copy(way, tile).start())
        return carry

    lax.fori_loop(0, tiles, spread, 0)

    row_iota = lax.broadcasted_iota(jnp.int32, (STRIP, LANES), 0)
    grid_row = row_iota + (me * rows - OWN_FIRST)
    inside = (grid_row >= 0) & (grid_row < rows * columns)

    def prepare(tile):
        for way, heard in ((0, me >= 2), (1, odd), (2, ~odd), (3, me + 2 < columns)):
            @pl.when(heard)
            def _():
                phase_copy(way, tile).wait_recv()
        s, c = sin_cos(ph[tile])
        objr[tile + 1] = jnp.where(inside, c, 0.0)
        obji[tile + 1] = jnp.where(inside, s, 0.0)

    def finish(tile):
        ways(lambda way: grad_copy(way, tile).wait_recv(), -1)
        total = gacc[tile + 1, OWN_FIRST : OWN_FIRST + rows]
        row = lax.broadcasted_iota(jnp.int32, (rows, LANES), 0)
        for way, (offset, lo, hi, at) in enumerate(GRAD_MOVES):
            ok = (row >= at) & (row < at + hi - lo) & there(-offset)
            total = total + jnp.where(ok, cbuf[way, tile], 0.0)
        gbuf[0, tile] = total
        for step in range(1, groups):
            share_copy(step, tile).start()

    lane = lax.broadcasted_iota(jnp.int32, (STRIP, LANES), 1)
    row16 = lax.broadcasted_iota(jnp.int32, (STRIP - PATCH, LANES), 0)
    extra = STRIP - PATCH

    def restack(x):
        upper = jnp.concatenate([x[:PATCH, :PATCH], x[PATCH:, :PATCH]], 1)
        lower = jnp.concatenate([x[:PATCH, PATCH:], x[PATCH:, PATCH:]], 1)
        return jnp.concatenate([upper, lower], 0)

    def shift_of(p, half):
        position = 2 * p + half
        return jit_ref[0, position], jit_ref[1, position] + (PATCH - 40 if half == 0 else PATCH // 2 - 40)

    def forward(p):
        slot = p % 2
        waves = []
        for half in range(2):
            jr, start = shift_of(p, half)
            keep = lane >= start

            def wrapped(image):
                tall = jnp.where(keep, image[p + half], image[p + half + 1])
                top = jnp.where(row16 >= jr, tall[:extra], tall[PATCH:])
                return jnp.concatenate([top, tall[extra:PATCH]], 0)

            o_r, o_i = wrapped(objr), wrapped(obji)
            p_r = pltpu.roll(pltpu.roll(probe_ref[0], jr, 0), start, 1)
            p_i = pltpu.roll(pltpu.roll(probe_ref[1], jr, 0), start, 1)
            waves.append(jnp.concatenate([p_r * o_r - p_i * o_i, p_r * o_i + p_i * o_r], 0))
            for index, value in enumerate((o_r, o_i, p_r, p_i)):
                own_ref[slot, half, index] = value
        wave = jnp.concatenate(waves, 1)
        wave_ref[slot] = wave
        far = from_right(restack(from_left(th_ref[...], tl_ref[...], wave)), rh_ref[...], rl_ref[...])
        f_r, f_i = far[:, :PATCH], far[:, PATCH:]
        square = f_r * f_r + f_i * f_i
        inverse = lax.rsqrt(jnp.maximum(square, (1e-35)))
        target = meas_ref[2 * p : 2 * p + 2].reshape(2 * PATCH, PATCH).astype(F32)
        error = square * inverse - target
        ratio = target * jnp.minimum(inverse, (1.0 / floor_value))
        level_ref[slot] = jnp.concatenate([ratio * f_r, ratio * f_i], 1)
        return jnp.sum((error * error).reshape(2 * PATCH // 8, 8, PATCH), axis=0)

    def backward(p):
        slot = p % 2
        back = from_left(rh_ref[...], rl_ref[...], restack(from_right(level_ref[slot], th_ref[...], tl_ref[...])))
        diff = back - wave_ref[slot]
        parts = []
        for half in range(2):
            jr, start = shift_of(p, half)
            keep = lane >= start
            d = diff[:, half * PATCH : (half + 1) * PATCH]
            d_r, d_i = d[:PATCH], d[PATCH:]
            o_r, o_i, p_r, p_i = (own_ref[slot, half, index] for index in range(4))
            c_re = p_r * d_r + p_i * d_i
            c_im = p_r * d_i - p_i * d_r
            g = o_r * c_im - o_i * c_re
            below = row16 >= jr
            tall = jnp.concatenate(
                [jnp.where(below, g[:extra], 0.0), g[extra:], jnp.where(below, 0.0, g[:extra])], 0
            )
            parts.append((jnp.where(keep, tall, 0.0), jnp.where(keep, 0.0, tall)))
        gacc[p] = gacc[p] + parts[0][0]
        gacc[p + 1] = gacc[p + 1] + (parts[0][1] + parts[1][0])
        gacc[p + 2] = parts[1][1]

    def near_copy(step):
        return remote(mis1.at[near_id], mis1.at[near_id], m1_s.at[step - 1], m1_r.at[step - 1], near_device(step))

    def far_copy(step):
        return remote(mis2.at[my_far], mis2.at[my_far], m2_s.at[step - 1], m2_r.at[step - 1], far_device(step))

    relay(0)
    relay(1)
    prepare(0)
    relay(2)
    prepare(1)
    for load in loads[1:]:
        load.wait()
    misfit = forward(0)
    for p in range(tiles):
        if p + 3 < tiles:
            relay(p + 3)
        if p + 2 < tiles:
            prepare(p + 2)
        backward(p)
        if p + 1 < tiles:
            misfit = misfit + forward(p + 1)
        if p >= 1:
            ways(lambda way: grad_copy(way, p - 1).start(), 1)
        if p == tiles - 2:
            mis1[near_id] = jnp.sum(misfit, axis=0, keepdims=True)
            for step in range(1, near_all):
                near_copy(step).start()
        if p >= 5:
            finish(p - 5)
    ways(lambda way: grad_copy(way, tiles - 1).start(), 1)
    for step in range(1, near_all):
        near_copy(step).wait_recv()
    mis2[my_far] = jnp.sum(mis1[...], axis=0)
    for step in range(1, far_count):
        far_copy(step).start()
    finish(tiles - 5)
    finish(tiles - 4)
    finish(tiles - 3)
    finish(tiles - 2)
    finish(tiles - 1)

    def collect(tile, carry):
        for step in range(1, groups):
            angle_copy(step, tile).wait_send()
            share_copy(step, tile).wait_send()
        sent(lambda way: phase_copy(way, tile).wait_send())
        relayed(lambda first, copy: copy.wait_send(), tile)
        ways(lambda way: grad_copy(way, tile).wait_send(), 1)
        return carry

    for tile in range(tiles):
        span = slice(tile * LANES, (tile + 1) * LANES)
        news = [jnp.zeros((rows, LANES), F32)] * layers
        for step in range(groups):
            if step > 0:
                share_copy(step, tile).wait_recv()
            angle = lax.rem(group - step + groups, groups)
            for layer in range(layers):
                news[layer] = news[layer] + (step_ref[angle] * path_ref[angle, group, layer]) * gbuf[step, tile]
        for layer in range(layers):
            new_out[0, layer, :, span] = news[layer]
    for step in range(1, near_all):
        near_copy(step).wait_send()
    for step in range(1, far_count):
        far_copy(step).wait_recv()
    total = jnp.sum(mis2[...], axis=0)
    mis_out[...] = jnp.sum(total, keepdims=True)
    for step in range(1, far_count):
        far_copy(step).wait_send()
    lax.fori_loop(0, tiles, collect, 0)


def body(mesh, volume, path_lengths, probe, measured, jitter, step_sizes):
    groups, columns = mesh.shape["blk"], mesh.shape["wide"]
    near = math.gcd(columns, 4)
    slab = volume[0]
    layers, rows, cols = slab.shape
    tiles = cols // LANES
    tables = [jnp.asarray(t) for t in dft_tables(probe.shape[-1])]
    vmem = pl.BlockSpec(memory_space=pltpu.VMEM)
    smem = pl.BlockSpec(memory_space=pltpu.SMEM)
    hbm = pl.BlockSpec(memory_space=pl.ANY)
    sem = pltpu.SemaphoreType.DMA
    loaded = [slab, probe, measured[0, 0], *tables]
    others = max(groups - 1, 1)
    new, misfit = pl.pallas_call(
        functools.partial(kernel, groups, columns, near),
        out_shape=(
            jax.ShapeDtypeStruct((1, layers, rows, cols), F32),
            jax.ShapeDtypeStruct((1, 1), F32),
        ),
        in_specs=[smem] * 3 + [hbm] * 7,
        out_specs=(vmem, vmem),
        scratch_shapes=[
            *(pltpu.VMEM(x.shape, x.dtype) for x in loaded),
            sem((len(loaded),)),
            pltpu.VMEM((2, 2 * PATCH, 2 * PATCH), F32),
            pltpu.VMEM((2, 2 * PATCH, 2 * PATCH), F32),
            pltpu.VMEM((2, 2, 4, PATCH, PATCH), F32),
            pltpu.VMEM((others, tiles, rows, LANES), F32),
            pltpu.VMEM((others, tiles, rows, LANES), F32),
            pltpu.VMEM((tiles, STRIP, LANES), F32),
            pltpu.VMEM((tiles + 2, STRIP, LANES), F32),
            pltpu.VMEM((tiles + 2, STRIP, LANES), F32),
            pltpu.VMEM((tiles + 2, STRIP, LANES), F32),
            pltpu.VMEM((4, tiles, rows, LANES), F32),
            pltpu.VMEM((groups, tiles, rows, LANES), F32),
            pltpu.VMEM((groups * near, 1, LANES), F32),
            pltpu.VMEM((columns // near, 1, LANES), F32),
            sem((others, tiles)), sem((others, tiles)),
            sem((4, tiles)), sem((4, tiles)),
            sem((4, tiles)), sem((4, tiles)),
            sem((others, tiles)), sem((others, tiles)),
            sem((groups * near,)), sem((groups * near,)),
            sem((columns // near,)), sem((columns // near,)),
        ],
        compiler_params=pltpu.CompilerParams(collective_id=0, has_side_effects=True),
    )(path_lengths, jitter[:, 0, 0], step_sizes, *loaded)
    return (volume - new, misfit[0, 0])


def solution(mesh):
    in_specs = (
        P("blk", None, "wide", None),
        P(),
        P(),
        P("blk", "wide", None, None, None),
        P(None, "blk", "wide", None),
        P(),
    )
    out_specs = (P("blk", None, "wide", None), P())
    return jax.shard_map(
        functools.partial(body, mesh), mesh=mesh, in_specs=in_specs, out_specs=out_specs, check_vma=False
    )
```
